512 devices in a mesh: parts: 2 (over y), tok: 32 (over z), hid: 8 (over x, core).
Axes of the slice: x: 4, y: 2, z: 32, core: 2. Of those that a mesh axis runs over, the one named last changes fastest.
The devices are a block of a 4x8x32 slice.
Arguments:
- tokens: bfloat16 [49152, 8192], P(('parts', 'tok'), 'hid'), parts along dimension 0, may hold values from -6 to 6
- adapter_ids: int32 [49152, 1], P(('parts', 'tok')), parts along dimension 0, may hold values from 0 to 255; in each aligned block of 768 rows (0 to 767, 768 to 1535, ...) at most 9 rows name the same one
- value_weight: bfloat16 [8192, 1024], P('hid'), may hold values from -0.0625 to 0.0625
- adapter_down: bfloat16 [256, 16, 8192], P('tok', None, 'hid'), may hold values from -0.0625 to 0.0625
- adapter_up: bfloat16 [256, 16, 1024], P('tok', None, 'hid'), may hold values from -1.5 to 1.5
Outputs:
- value_out: bfloat16 [49152, 1024], P(('parts', 'tok'), 'hid'), parts along dimension 0
The draws below stay inside these ranges and needn't reach their ends.
There are 2 independent parts, one for each index of `parts`. The reference program is written for one: setup_inputs(seed, part) draws one part's arguments, and reference() takes and returns one part's arrays. A program takes and returns all parts, laid end to end along the dimension named above; an argument that names none is the same for every part. Nothing has to cross between parts.
Inputs may be any that keep to these rules, and one draw needn't show every extreme that they name: `adapter_ids`: among the 768 tokens of one index of tok, each adapter id appears at most 9 times; in some of these aligned blocks one id appears exactly 9 times.
All inputs are finite; a program needn't handle non-finite values.
Results may differ from the reference program's by a relative error of at most 0.0048.
Values may be sent and summed in bfloat16 or wider, within the bound.
No kernel may reach another device: no remote copies, remote signals or barrier semaphores. Data moves between devices by JAX's collectives and lax.ppermute only.
A program may use at most 128 MiB of HBM per device.

```python
import math
import jax
import jax.numpy as jnp
import numpy as np
from jax import lax

D = 8192
KV = 1024
R = 16
TOK_DEV = 768
ADAPTERS = 256
CAP = 9
TOKENS = 24576


def levels(own_key, dims, shards, smallest, high):
    gain, own = 1.0, jax.random.fold_in(own_key, 6)
    for position, shards_of in shards:
        steps = jnp.exp(jax.random.uniform(jax.random.fold_in(own, position), (shards_of,), jnp.float32, smallest / len(shards), high / len(shards)))
        gain = gain * jnp.repeat(steps, dims[position] // shards_of).reshape([-1 if axis == position else 1 for axis in range(len(dims))])
    return gain


def routed_block(key, own, number, rows, number_of, top, reach, lean):
    ranking = jax.random.permutation(key, number_of)
    heavy_load, common = portions_of(number_of, rows * top, reach, lean, True), portions_of(number_of, rows * top, reach, lean, False)
    places = jnp.arange(number_of)

    def named(tallies, offset_by):
        used = int((tallies > 0).sum())
        fixed = max(1, used // 4)
        moved = fixed + (places - fixed + offset_by * (used - fixed)) % max(1, number_of - fixed)
        return jnp.zeros((number_of,), jnp.int32).at[ranking[jnp.where(places < fixed, places, moved)]].set(jnp.asarray(tallies, jnp.int32))

    tallies = jnp.where(number % 4 == 0, named(heavy_load, number // 4), named(common, number - number // 4 - 1))
    mixed = jax.random.permutation(jax.random.fold_in(own, 3), number_of)
    source_of, receiver = mixed[0:number_of // 2 * 2:2], mixed[1:number_of // 2 * 2:2]
    slack = jnp.minimum(tallies[source_of] - 1, reach - tallies[receiver]) // 2
    slack = jnp.where((source_of == ranking[0]) | (receiver == ranking[0]) | (tallies[receiver] == 0), 0, jnp.maximum(slack, 0))
    moved = jax.random.randint(jax.random.fold_in(own, 4), (number_of // 2,), 0, 1 << 20) % (slack + 1)
    tallies = tallies.at[source_of].add(-moved).at[receiver].add(moved)
    labels = jnp.searchsorted(jnp.cumsum(tallies), jnp.arange(rows * top), side="right").astype(jnp.int32)
    listing = labels.reshape(top, rows).T
    listing = listing[jax.random.permutation(jax.random.fold_in(own, 1), rows)]
    offset_by = jax.random.randint(jax.random.fold_in(own, 2), (rows, 1), 0, top)
    return jnp.take_along_axis(listing, (jnp.arange(top)[None, :] + offset_by) % top, axis=1)


def portions_of(number_of, total, limit, slope, full):
    portions = [(1 << 20) // math.isqrt(grade ** slope) + 1 for grade in range(1, number_of + 1)]
    largest = limit if full else min(limit, max(-(-total // number_of), total * portions[0] // sum(portions)))
    least = 1 if total - largest >= number_of - 1 else 0
    holding, spare = [largest] + [least] * (number_of - 1), total - largest - least * (number_of - 1)
    while spare > 0:
        candidates = [i for i in range(1, number_of) if holding[i] < largest] or [i for i in range(1, number_of) if holding[i] < limit]
        mass, remaining = sum([portions[i] for i in candidates]), spare
        for i in candidates:
            extra = min(limit - holding[i], max(1, remaining * portions[i] // mass), spare)
            holding[i] = holding[i] + extra
            spare = spare - extra
    return np.array(holding)


def noise(key, extent, scale, most, cuts=(), held_as=jnp.bfloat16):
    result = scale * jax.random.normal(key, extent, jnp.float32)
    if cuts:
        result = result * levels(key, extent, cuts, -0.22, 0.18)
    return jnp.clip(result, -most, most).astype(held_as)


def setup_inputs(seed: int = 0, part: int = 0) -> dict:
    seeds = jax.random.split(jax.random.key(seed), 6)
    part_keys = jax.random.split(jax.random.fold_in(seeds[5], part), 6)
    tokens = noise(part_keys[0], (TOKENS, D), 1.0, 6.0, ((0, 32), (1, 8)))
    adapter_ids_keys = jax.random.split(jax.random.fold_in(part_keys[1], 1), TOKENS // TOK_DEV)
    adapter_ids_turns = jax.random.permutation(jax.random.fold_in(part_keys[1], 3), TOKENS // TOK_DEV)
    adapter_ids = jax.vmap(lambda own, number: routed_block(jax.random.fold_in(part_keys[1], 2), own, number, TOK_DEV, ADAPTERS, 1, CAP, 2))(adapter_ids_keys, adapter_ids_turns).reshape((TOKENS, 1))
    value_weight = noise(seeds[2], (D, KV), D ** -0.5, 0.0625, ((0, 8),))
    adapter_down = noise(seeds[3], (ADAPTERS, R, D), D ** -0.5, 0.0625, ((0, 32), (2, 8)))
    adapter_up = noise(seeds[4], (ADAPTERS, R, KV), R ** -0.5, 1.5, ((0, 32), (2, 8)))
    return {"tokens": tokens, "adapter_ids": adapter_ids, "value_weight": value_weight, "adapter_down": adapter_down, "adapter_up": adapter_up}


def reference(tokens, adapter_ids, value_weight, adapter_down, adapter_up):
    base_sums = jnp.dot(tokens, value_weight, preferred_element_type=jnp.float32)
    block_rows = math.gcd(TOKENS, 512)
    block_count = TOKENS // block_rows
    token_blocks = tokens.reshape(block_count, block_rows, D)
    id_blocks = adapter_ids[:, 0].reshape(block_count, block_rows)

    def block_delta(block_args):
        rows_block, ids_block = block_args
        down_picked = adapter_down[ids_block].astype(jnp.float32)
        low_rows = jnp.einsum("td,trd->tr", rows_block.astype(jnp.float32), down_picked).astype(jnp.bfloat16)
        up_picked = adapter_up[ids_block].astype(jnp.float32)
        return jnp.einsum("tr,trk->tk", low_rows.astype(jnp.float32), up_picked).astype(jnp.bfloat16)

    delta_rows = lax.map(block_delta, (token_blocks, id_blocks)).reshape(TOKENS, KV)
    return (base_sums + delta_rows.astype(jnp.float32)).astype(jnp.bfloat16)
```

```python
import functools

import jax
import jax.numpy as jnp
from jax import lax
from jax.experimental import pallas as pl
from jax.experimental.pallas import tpu as pltpu
from jax.sharding import PartitionSpec as P

VMEM = pl.BlockSpec(memory_space=pltpu.VMEM)
SMEM = pl.BlockSpec(memory_space=pltpu.SMEM)


def low_kernel(low_rank, tile, first_ref, *refs):
    *pieces, mine_ref, other_ref, key_ref, acc_ref, out_ref = refs
    half = pieces[0].shape[0] // 2
    d_local = mine_ref.shape[1]

    def one_tile(i, carry):
        cols = pl.ds(pl.multiple_of(i * tile, tile), tile)
        key = key_ref[:, cols]
        total = acc_ref[:, cols]
        for n, piece in enumerate(pieces):
            found = lax.dot_general(
                piece[:half, :d_local],
                mine_ref[cols, :],
                (((1,), (1,)), ((), ())),
                preferred_element_type=jnp.float32,
            ) + lax.dot_general(
                piece[half:, :d_local],
                other_ref[cols, :],
                (((1,), (1,)), ((), ())),
                preferred_element_type=jnp.float32,
            )
            for g in range(half // low_rank):
                hit = key == first_ref[0] + (n * (half // low_rank) + g)
                total = total + jnp.where(hit, found[g * low_rank : (g + 1) * low_rank], 0.0)
        out_ref[:, cols] = total
        return carry

    lax.fori_loop(0, mine_ref.shape[0] // tile, one_tile, 0)


def low_add(low_rank, first, pieces, mine, other, key, acc):
    tok_rows, d_local = mine.shape
    rows = sum(p.shape[0] for p in pieces)
    tile = 256 if tok_rows % 256 == 0 else tok_rows
    return pl.pallas_call(
        functools.partial(low_kernel, low_rank, tile),
        out_shape=jax.ShapeDtypeStruct(acc.shape, acc.dtype),
        in_specs=[SMEM] + [VMEM] * (len(pieces) + 4),
        out_specs=VMEM,
        cost_estimate=pl.CostEstimate(
            flops=2 * rows * d_local * tok_rows,
            bytes_accessed=2 * rows * d_local,
            transcendentals=0,
        ),
        compiler_params=pltpu.CompilerParams(vmem_limit_bytes=24 * 2**20),
    )(first, *pieces, mine, other, key, acc)


def delta_kernel(
    low_rank, first_ref, low_ref, key_ref, far_key_ref, up_ref, far_ref, base_ref, out_ref, acc_ref
):
    low = jnp.sum(low_ref[...], axis=0).astype(jnp.bfloat16)
    tok_rows = low.shape[1]
    piece_rows = 64
    per_piece = piece_rows // low_rank
    n_pieces = up_ref.shape[0] // piece_rows
    acc_ref[...] = jnp.zeros_like(acc_ref)
    for table, key_of, which in ((up_ref, key_ref, 0), (far_ref, far_key_ref, 1)):
        key = key_of[...]

        def pair(j, carry):
            groups = []
            for n in range(4):
                i = 4 * j + n
                first = jnp.where(
                    i == 0,
                    first_ref[which],
                    jnp.where(
                        i == n_pieces - 1, per_piece * (i + 1) + first_ref[which], per_piece * (i + 1)
                    ),
                )
                for g in range(per_piece):
                    hit = jnp.where(key == first + g, 1.0, 0.0).astype(jnp.bfloat16)
                    groups.append(low * hit)
            spread = jnp.concatenate(groups, axis=0)
            rows = pl.ds(pl.multiple_of(j * 4 * piece_rows, 4 * piece_rows), 4 * piece_rows)
            acc_ref[...] += lax.dot_general(
                table[rows, :],
                spread,
                (((0,), (0,)), ((), ())),
                preferred_element_type=jnp.float32,
            )
            return carry

        lax.fori_loop(0, n_pieces // 4, pair, 0)
    delta = acc_ref[...].astype(jnp.bfloat16).astype(jnp.float32)
    out_ref[...] = (base_ref[...] + delta).T.astype(jnp.bfloat16)


def delta_add(low_rank, first, low_all, key, far_key, up, far, base):
    kv_local, tok_rows = base.shape
    return pl.pallas_call(
        functools.partial(delta_kernel, low_rank),
        out_shape=jax.ShapeDtypeStruct((tok_rows, kv_local), jnp.bfloat16),
        in_specs=[SMEM] + [VMEM] * 6,
        out_specs=VMEM,
        scratch_shapes=[pltpu.VMEM((kv_local, tok_rows), jnp.float32)],
        cost_estimate=pl.CostEstimate(
            flops=4 * up.shape[0] * kv_local * tok_rows,
            bytes_accessed=8 * up.shape[0] * kv_local,
            transcendentals=0,
        ),
        compiler_params=pltpu.CompilerParams(vmem_limit_bytes=24 * 2**20),
    )(first, low_all, key, far_key, up, far, base)


def per_device(tokens, adapter_ids, value_weight, adapter_down, adapter_up):
    tok_rows, d_local = tokens.shape
    n_tok = lax.axis_size("tok")
    n_hid = lax.axis_size("hid")
    adp_dev, low_rank, _ = adapter_down.shape
    kv_local = adapter_up.shape[2]
    rows = adp_dev * low_rank
    half = rows // 2
    half_adp = adp_dev // 2
    f32 = jnp.float32
    me = lax.axis_index("tok")
    side = lax.axis_index("hid") % 2
    token_ids = adapter_ids[:, 0][None, :]

    swap = [(h, h ^ 1) for h in range(n_hid)]
    onward = []
    for t in range(n_tok):
        for h in range(n_hid):
            onward.append((t * n_hid + h, ((t + 1 - 2 * (h % 2)) % n_tok) * n_hid + h))

    block = jnp.concatenate(
        [adapter_down.reshape(rows, d_local), adapter_up.reshape(rows, kv_local)], axis=1
    )
    block_other = lax.ppermute(block, "hid", swap)
    flight = [
        jnp.concatenate([block[:half], block_other[:half]], axis=0),
        jnp.concatenate([block[half:], block_other[half:]], axis=0),
    ]
    flight[0], flight[1], tokens = lax.optimization_barrier((flight[0], flight[1], tokens))
    own = jnp.where(side == 0, flight[0], flight[1])
    tokens_other = lax.ppermute(tokens, "hid", swap)
    partial_base = lax.dot_general(
        value_weight, tokens, (((0,), (1,)), ((), ())), preferred_element_type=f32
    )

    owner, slot = token_ids // adp_dev, token_ids % adp_dev
    behind = jnp.where(me >= owner, me - owner, me - owner + n_tok)
    ahead = jnp.where(owner >= me, owner - me, owner - me + n_tok)
    key = jnp.where(side == 0, behind, ahead) * adp_dev + slot
    far_key = jnp.where(side == 0, ahead, behind) * adp_dev + slot

    def first_at(step, extra=0):
        return jnp.full((1,), step * adp_dev, jnp.int32) + extra

    low = low_add(
        low_rank,
        first_at(0, side * half_adp),
        [own],
        tokens,
        tokens_other,
        key,
        jnp.zeros((low_rank, tok_rows), f32),
    )
    ups = [own]
    base_blocks = None
    for step in range(1, n_tok // 2):
        for c in range(2):
            flight[c] = lax.ppermute(flight[c], ("tok", "hid"), onward)
            ups.append(flight[c])
        if step > 3:
            flight[1], low = lax.optimization_barrier((flight[1], low))
        low = low_add(low_rank, first_at(step), list(flight), tokens, tokens_other, key, low)
        if step == 1:
            base_blocks = lax.all_to_all(
                partial_base.reshape(n_hid, kv_local, tok_rows), "hid", 0, 0, tiled=True
            )
    last = lax.ppermute(jnp.where(side == 0, flight[0], flight[1]), ("tok", "hid"), onward)
    ups.append(last)
    low = low_add(
        low_rank,
        first_at(n_tok // 2, side * half_adp),
        [last],
        tokens,
        tokens_other,
        key,
        low,
    )
    low_all = lax.all_to_all(
        jnp.broadcast_to(low[None], (n_hid, *low.shape)), "hid", 0, 0, tiled=True
    )
    up_mine = jnp.concatenate([u[:half, d_local:] for u in ups], axis=0)
    up_far = lax.ppermute(
        jnp.concatenate([u[half:, d_local:] for u in ups], axis=0), "hid", swap
    )
    base = jnp.sum(base_blocks, axis=0)
    return delta_add(
        low_rank,
        jnp.stack([side * half_adp, (1 - side) * half_adp]),
        low_all,
        key,
        far_key,
        up_mine,
        up_far,
        base,
    )


def solution(mesh):
    in_specs = (
        P(("parts", "tok"), "hid"),
        P(("parts", "tok"), None),
        P("hid", None),
        P("tok", None, "hid"),
        P("tok", None, "hid"),
    )
    out_specs = P(("parts", "tok"), "hid")
    return jax.shard_map(
        per_device, mesh=mesh, in_specs=in_specs, out_specs=out_specs, check_vma=False
    )
```

```python
import functools

import jax
import jax.numpy as jnp
from jax import lax
from jax.experimental import pallas as pl
from jax.experimental.pallas import tpu as pltpu
from jax.sharding import PartitionSpec as P

VMEM = pl.BlockSpec(memory_space=pltpu.VMEM)
LOW_VMEM = 12 * 2**20


def low_kernel(low_rank, count, first, *refs):
    pieces = refs[:count]
    mine_ref, other_ref, key_ref, acc_ref, out_ref, up_ref, far_ref = refs[count:]
    half = pieces[0].shape[0] // 2
    d_local = mine_ref.shape[1]
    found = lax.dot_general(
        jnp.concatenate([p[:half, :d_local] for p in pieces], axis=0),
        mine_ref[...],
        (((1,), (1,)), ((), ())),
        preferred_element_type=jnp.float32,
    ) + lax.dot_general(
        jnp.concatenate([p[half:, :d_local] for p in pieces], axis=0),
        other_ref[...],
        (((1,), (1,)), ((), ())),
        preferred_element_type=jnp.float32,
    )
    key = key_ref[...]
    total = acc_ref[...]
    for g in range(found.shape[0] // low_rank):
        total = total + jnp.where(
            key == first + g, found[g * low_rank : (g + 1) * low_rank], 0.0
        )
    out_ref[...] = jnp.broadcast_to(total, out_ref.shape)
    for n, p in enumerate(pieces):
        up_ref[n * half : (n + 1) * half] = p[:half, d_local:]
        far_ref[n * half : (n + 1) * half] = p[half:, d_local:]


def low_add(low_rank, first, pieces, mine, other, key, acc, copies):
    tok_rows, d_local = mine.shape
    piece_rows, width = pieces[0].shape
    half = len(pieces) * piece_rows // 2
    table = jax.ShapeDtypeStruct((half, width - d_local), jnp.bfloat16)
    return pl.pallas_call(
        functools.partial(low_kernel, low_rank, len(pieces), first),
        out_shape=(jax.ShapeDtypeStruct(copies + acc.shape, acc.dtype), table, table),
        in_specs=[VMEM] * (len(pieces) + 4),
        out_specs=(VMEM, VMEM, VMEM),
        cost_estimate=pl.CostEstimate(
            flops=4 * half * d_local * tok_rows,
            bytes_accessed=4 * half * d_local,
            transcendentals=0,
        ),
        compiler_params=pltpu.CompilerParams(vmem_limit_bytes=LOW_VMEM),
    )(*pieces, mine, other, key, acc)


def join_kernel(*refs):
    *parts, out_ref = refs
    at = 0
    for p in parts:
        out_ref[at : at + p.shape[0]] = p[...]
        at += p.shape[0]


def join(parts):
    return pl.pallas_call(
        join_kernel,
        out_shape=jax.ShapeDtypeStruct(
            (sum(p.shape[0] for p in parts), parts[0].shape[1]), parts[0].dtype
        ),
        in_specs=[VMEM] * len(parts),
        out_specs=VMEM,
        compiler_params=pltpu.CompilerParams(vmem_limit_bytes=LOW_VMEM),
    )(*parts)


def sum_kernel(blocks_ref, out_ref):
    out_ref[...] = jnp.sum(blocks_ref[...], axis=0)


def sum_blocks(blocks):
    return pl.pallas_call(
        sum_kernel,
        out_shape=jax.ShapeDtypeStruct(blocks.shape[1:], blocks.dtype),
        in_specs=[VMEM],
        out_specs=VMEM,
        cost_estimate=pl.CostEstimate(
            flops=blocks.size, bytes_accessed=4 * blocks.size, transcendentals=0
        ),
        compiler_params=pltpu.CompilerParams(vmem_limit_bytes=LOW_VMEM),
    )(blocks)


def delta_kernel(low_rank, adp_dev, low_ref, key_ref, far_key_ref, *refs):
    *ups, far_ref, base_ref, out_ref = refs
    low = jnp.sum(low_ref[...], axis=0).astype(jnp.bfloat16)
    half = adp_dev // 2 * low_rank
    acc = jnp.zeros(base_ref.shape, jnp.float32)

    def expand(key, table, row):
        groups = []
        for at in range(0, table.shape[0], low_rank):
            adapter = (row + at) // low_rank
            if row + at >= half:
                adapter += adp_dev // 2
            groups.append(low * jnp.where(key == adapter, 1.0, 0.0).astype(jnp.bfloat16))
        return lax.dot_general(
            table,
            jnp.concatenate(groups, axis=0),
            (((0,), (0,)), ((), ())),
            preferred_element_type=jnp.float32,
        )

    row = 0
    for up in ups:
        acc += expand(key_ref[...], up[...], row)
        row += up.shape[0]
    row = 0
    for up in ups:
        acc += expand(far_key_ref[...], far_ref[row : row + up.shape[0]], row)
        row += up.shape[0]
    delta = acc.astype(jnp.bfloat16).astype(jnp.float32)
    out_ref[...] = (base_ref[...] + delta).T.astype(jnp.bfloat16)


def delta_add(low_rank, adp_dev, low_all, key, far_key, ups, far, base):
    kv_local, tok_rows = base.shape
    return pl.pallas_call(
        functools.partial(delta_kernel, low_rank, adp_dev),
        out_shape=jax.ShapeDtypeStruct((tok_rows, kv_local), jnp.bfloat16),
        in_specs=[VMEM] * (5 + len(ups)),
        out_specs=VMEM,
        cost_estimate=pl.CostEstimate(
            flops=4 * far.shape[0] * kv_local * tok_rows,
            bytes_accessed=8 * far.shape[0] * kv_local,
            transcendentals=0,
        ),
        compiler_params=pltpu.CompilerParams(vmem_limit_bytes=24 * 2**20),
    )(low_all, key, far_key, *ups, far, base)


def per_device(tokens, adapter_ids, value_weight, adapter_down, adapter_up):
    tok_rows, d_local = tokens.shape
    n_tok = lax.axis_size("tok")
    n_hid = lax.axis_size("hid")
    adp_dev, low_rank, _ = adapter_down.shape
    kv_local = adapter_up.shape[2]
    rows = adp_dev * low_rank
    half = rows // 2
    half_adp = adp_dev // 2
    f32 = jnp.float32
    me = lax.axis_index("tok")
    side = lax.axis_index("hid") % 2
    token_ids = adapter_ids[:, 0][None, :]

    swap = [(h, h ^ 1) for h in range(n_hid)]
    onward = []
    for t in range(n_tok):
        for h in range(n_hid):
            onward.append((t * n_hid + h, ((t + 1 - 2 * (h % 2)) % n_tok) * n_hid + h))

    block = jnp.concatenate(
        [adapter_down.reshape(rows, d_local), adapter_up.reshape(rows, kv_local)], axis=1
    )
    block_other = lax.ppermute(block, "hid", swap)
    top = jnp.concatenate([block[:half], block_other[:half]], axis=0)
    bottom = jnp.concatenate([block[half:], block_other[half:]], axis=0)
    flight = [jnp.where(side == 0, top, bottom), jnp.where(side == 0, bottom, top)]
    flight[0], flight[1], tokens = lax.optimization_barrier((flight[0], flight[1], tokens))
    own = flight[0]
    tokens_other = lax.ppermute(tokens, "hid", swap)
    partial_base = lax.dot_general(
        value_weight, tokens, (((0,), (1,)), ((), ())), preferred_element_type=f32
    )

    owner, slot = token_ids // adp_dev, token_ids % adp_dev
    behind = jnp.where(me >= owner, me - owner, me - owner + n_tok)
    ahead = jnp.where(owner >= me, owner - me, owner - me + n_tok)
    turned = (slot + half_adp) % adp_dev
    key = jnp.where(side == 0, behind * adp_dev + slot, ahead * adp_dev + turned)
    far_key = jnp.where(side == 0, ahead * adp_dev + turned, behind * adp_dev + slot)

    def add(low, step, pieces, copies=()):
        low, up, far = low_add(
            low_rank, step * adp_dev, pieces, tokens, tokens_other, key, low, copies
        )
        ups.append(up)
        fars.append(far)
        return low

    ups, fars, waiting = [], [], []
    low = add(jnp.zeros((low_rank, tok_rows), f32), 0, [own])
    for step in range(1, n_tok // 2):
        for c in range(2):
            flight[c] = lax.ppermute(flight[c], ("tok", "hid"), onward)
        waiting += flight
        if step == 2:
            flight[1], partial_base = lax.optimization_barrier((flight[1], partial_base))
            base_blocks = lax.all_to_all(
                partial_base.reshape(n_hid, kv_local, tok_rows), "hid", 0, 0, tiled=True
            )
        if step == 10:
            flight[1], base_blocks = lax.optimization_barrier((flight[1], base_blocks))
            base = sum_blocks(base_blocks)
        if step % 2 == 0 or step == n_tok // 2 - 1:
            if step > 2:
                flight[1], low = lax.optimization_barrier((flight[1], low))
            low = add(low, step - len(waiting) // 2 + 1, waiting)
            waiting = []
    last = lax.ppermute(flight[0], ("tok", "hid"), onward)
    low_copies = add(low, n_tok // 2, [last], (n_hid,))
    low_all = lax.all_to_all(low_copies, "hid", 0, 0, tiled=True)
    up_far = lax.ppermute(join(fars), "hid", swap)
    return delta_add(low_rank, adp_dev, low_all, key, far_key, ups, up_far, base)


def solution(mesh):
    in_specs = (
        P(("parts", "tok"), "hid"),
        P(("parts", "tok"), None),
        P("hid", None),
        P("tok", None, "hid"),
        P("tok", None, "hid"),
    )
    out_specs = P(("parts", "tok"), "hid")
    return jax.shard_map(
        per_device, mesh=mesh, in_specs=in_specs, out_specs=out_specs, check_vma=False
    )
```

```python
import functools

import jax
import jax.numpy as jnp
from jax import lax
from jax.experimental import pallas as pl
from jax.experimental.pallas import tpu as pltpu
from jax.sharding import PartitionSpec as P

VMEM = pl.BlockSpec(memory_space=pltpu.VMEM)
ANY = pl.BlockSpec(memory_space=pl.ANY)
LOW_VMEM = 12 * 2**20


def low_kernel(low_rank, count, first, row, *refs):
    pieces = refs[:count]
    mine_ref, other_ref, key_ref, acc_ref = refs[count : count + 4]
    out_ref, up_ref, far_ref, sem = refs[-4:]
    half = pieces[0].shape[0] // 2
    d_local = mine_ref.shape[1]
    copies = []
    for n, p in enumerate(pieces):
        for k, table in enumerate((up_ref, far_ref)):
            copies.append(
                pltpu.make_async_copy(
                    p.at[k * half : (k + 1) * half, d_local:],
                    table.at[row + n * half : row + (n + 1) * half],
                    sem.at[2 * n + k],
                )
            )
            copies[-1].start()
    found = lax.dot_general(
        jnp.concatenate([p[:half, :d_local] for p in pieces], axis=0),
        mine_ref[...],
        (((1,), (1,)), ((), ())),
        preferred_element_type=jnp.float32,
    ) + lax.dot_general(
        jnp.concatenate([p[half:, :d_local] for p in pieces], axis=0),
        other_ref[...],
        (((1,), (1,)), ((), ())),
        preferred_element_type=jnp.float32,
    )
    key = key_ref[...]
    total = acc_ref[...]
    for g in range(found.shape[0] // low_rank):
        total = total + jnp.where(
            key == first + g, found[g * low_rank : (g + 1) * low_rank], 0.0
        )
    out_ref[...] = jnp.broadcast_to(total.astype(out_ref.dtype), out_ref.shape)
    for copy in copies:
        copy.wait()


def low_add(low_rank, first, row, pieces, mine, other, key, acc, out, tables, table_shape):
    tok_rows, d_local = mine.shape
    count = len(pieces)
    half = count * pieces[0].shape[0] // 2
    return pl.pallas_call(
        functools.partial(low_kernel, low_rank, count, first, row),
        out_shape=(out, table_shape, table_shape),
        in_specs=[VMEM] * (count + 4) + [ANY] * len(tables),
        out_specs=(VMEM, ANY, ANY),
        scratch_shapes=[pltpu.SemaphoreType.DMA((2 * count,))],
        input_output_aliases={count + 4 + i: 1 + i for i in range(len(tables))},
        cost_estimate=pl.CostEstimate(
            flops=4 * half * d_local * tok_rows,
            bytes_accessed=4 * half * d_local,
            transcendentals=0,
        ),
        compiler_params=pltpu.CompilerParams(vmem_limit_bytes=LOW_VMEM),
    )(*pieces, mine, other, key, acc, *tables)


def base_kernel(width, tokens_ref, weight_ref, out_ref):
    step = 2 * width
    for at in range(0, weight_ref.shape[1], step):
        found = jnp.dot(
            tokens_ref[...], weight_ref[:, at : at + step], preferred_element_type=jnp.float32
        )
        out_ref[at // width] = found[:, :width]
        out_ref[at // width + 1] = found[:, width:]


def base_blocks_of(tokens, weight, width):
    rows, depth = tokens.shape
    return pl.pallas_call(
        functools.partial(base_kernel, width),
        out_shape=jax.ShapeDtypeStruct((weight.shape[1] // width, rows, width), jnp.float32),
        in_specs=[VMEM, VMEM],
        out_specs=VMEM,
        cost_estimate=pl.CostEstimate(
            flops=2 * rows * depth * weight.shape[1],
            bytes_accessed=8 * weight.size,
            transcendentals=0,
        ),
        compiler_params=pltpu.CompilerParams(vmem_limit_bytes=LOW_VMEM),
    )(tokens, weight)


def sum_kernel(blocks_ref, out_ref):
    out_ref[...] = jnp.sum(blocks_ref[...], axis=0)


def sum_blocks(blocks):
    return pl.pallas_call(
        sum_kernel,
        out_shape=jax.ShapeDtypeStruct(blocks.shape[1:], blocks.dtype),
        in_specs=[VMEM],
        out_specs=VMEM,
        cost_estimate=pl.CostEstimate(
            flops=blocks.size, bytes_accessed=4 * blocks.size, transcendentals=0
        ),
        compiler_params=pltpu.CompilerParams(vmem_limit_bytes=LOW_VMEM),
    )(blocks)


def delta_kernel(low_rank, adp_dev, low_ref, key_ref, far_key_ref, up_ref, far_ref, base_ref, out_ref):
    low = jnp.sum(low_ref[...].astype(jnp.float32), axis=0).astype(jnp.bfloat16)
    half = adp_dev // 2 * low_rank
    tile = 4 * half
    acc = jnp.zeros((base_ref.shape[1], base_ref.shape[0]), jnp.float32)
    for key, table in ((key_ref[...], up_ref), (far_key_ref[...], far_ref)):
        for row in range(0, table.shape[0], tile):
            groups = []
            for at in range(row, row + tile, low_rank):
                adapter = at // low_rank + (adp_dev // 2 if at >= half else 0)
                groups.append(low * jnp.where(key == adapter, 1.0, 0.0).astype(jnp.bfloat16))
            acc += lax.dot_general(
                table[row : row + tile],
                jnp.concatenate(groups, axis=0),
                (((0,), (0,)), ((), ())),
                preferred_element_type=jnp.float32,
            )
    delta = acc.astype(jnp.bfloat16).astype(jnp.float32)
    out_ref[...] = (base_ref[...] + delta.T).astype(jnp.bfloat16)


def delta_add(low_rank, adp_dev, low_all, key, far_key, up, far, base):
    tok_rows, kv_local = base.shape
    return pl.pallas_call(
        functools.partial(delta_kernel, low_rank, adp_dev),
        out_shape=jax.ShapeDtypeStruct((tok_rows, kv_local), jnp.bfloat16),
        in_specs=[VMEM] * 6,
        out_specs=VMEM,
        cost_estimate=pl.CostEstimate(
            flops=4 * far.shape[0] * kv_local * tok_rows,
            bytes_accessed=8 * far.shape[0] * kv_local,
            transcendentals=0,
        ),
        compiler_params=pltpu.CompilerParams(vmem_limit_bytes=24 * 2**20),
    )(low_all, key, far_key, up, far, base)


def per_device(tokens, adapter_ids, value_weight, adapter_down, adapter_up):
    tok_rows, d_local = tokens.shape
    n_tok = lax.axis_size("tok")
    n_hid = lax.axis_size("hid")
    adp_dev, low_rank, _ = adapter_down.shape
    kv_local = adapter_up.shape[2]
    rows = adp_dev * low_rank
    half = rows // 2
    half_adp = adp_dev // 2
    f32 = jnp.float32
    me = lax.axis_index("tok")
    side = lax.axis_index("hid") % 2
    token_ids = adapter_ids[:, 0][None, :]

    swap = [(h, h ^ 1) for h in range(n_hid)]
    onward = []
    for t in range(n_tok):
        for h in range(n_hid):
            onward.append((t * n_hid + h, ((t + 1 - 2 * (h % 2)) % n_tok) * n_hid + h))

    block = jnp.concatenate(
        [adapter_down.reshape(rows, d_local), adapter_up.reshape(rows, kv_local)], axis=1
    )
    block_other = lax.ppermute(block, "hid", swap)
    top = jnp.concatenate([block[:half], block_other[:half]], axis=0)
    bottom = jnp.concatenate([block[half:], block_other[half:]], axis=0)
    flight = [jnp.where(side == 0, top, bottom), jnp.where(side == 0, bottom, top)]
    flight[0], flight[1], tokens = lax.optimization_barrier((flight[0], flight[1], tokens))
    own = flight[0]
    tokens_other = lax.ppermute(tokens, "hid", swap)
    owner, slot = token_ids // adp_dev, token_ids % adp_dev
    behind = jnp.where(me >= owner, me - owner, me - owner + n_tok)
    ahead = jnp.where(owner >= me, owner - me, owner - me + n_tok)
    turned = (slot + half_adp) % adp_dev
    key = jnp.where(side == 0, behind * adp_dev + slot, ahead * adp_dev + turned)
    far_key = jnp.where(side == 0, ahead * adp_dev + turned, behind * adp_dev + slot)

    sums = jax.ShapeDtypeStruct((low_rank, tok_rows), f32)
    table_shape = jax.ShapeDtypeStruct((n_tok // 2 * rows, kv_local), jnp.bfloat16)

    def add(state, step, pieces, out=sums):
        low, *tables = state
        row = step * rows - half if step else 0
        return low_add(
            low_rank,
            step * adp_dev,
            row,
            pieces,
            tokens,
            tokens_other,
            key,
            low,
            out,
            tables,
            table_shape,
        )

    waiting = []
    state = add((jnp.zeros(sums.shape, f32),), 0, [own])
    for step in range(1, n_tok // 2):
        for c in range(2):
            flight[c] = lax.ppermute(flight[c], ("tok", "hid"), onward)
        waiting += flight
        if step == 1:
            flight[1], value_weight = lax.optimization_barrier((flight[1], value_weight))
            partial_base = base_blocks_of(tokens, value_weight, kv_local)
        if step == 3:
            flight[1], partial_base = lax.optimization_barrier((flight[1], partial_base))
            base_blocks = lax.all_to_all(partial_base, "hid", 0, 0, tiled=True)
        if step == 11:
            flight[1], base_blocks = lax.optimization_barrier((flight[1], base_blocks))
            base = sum_blocks(base_blocks)
        if step == 13:
            flight[1], base = lax.optimization_barrier((flight[1], base))
        if step % 2 == 0 or step == n_tok // 2 - 1:
            if step > 2:
                flight[1], state = lax.optimization_barrier((flight[1], state))
            state = add(state, step - len(waiting) // 2 + 1, waiting)
            waiting = []
    last = lax.ppermute(flight[0], ("tok", "hid"), onward)
    low_copies, up, far = add(
        state,
        n_tok // 2,
        [last],
        jax.ShapeDtypeStruct((n_hid, low_rank, tok_rows), jnp.bfloat16),
    )
    low_all = lax.all_to_all(low_copies, "hid", 0, 0, tiled=True)
    far = lax.ppermute(far, "hid", swap)
    return delta_add(low_rank, adp_dev, low_all, key, far_key, up, far, base)


def solution(mesh):
    in_specs = (
        P(("parts", "tok"), "hid"),
        P(("parts", "tok"), None),
        P("hid", None),
        P("tok", None, "hid"),
        P("tok", None, "hid"),
    )
    out_specs = P(("parts", "tok"), "hid")
    return jax.shard_map(
        per_device, mesh=mesh, in_specs=in_specs, out_specs=out_specs, check_vma=False
    )
```

```python
import functools

import jax
import jax.numpy as jnp
from jax import lax
from jax.experimental import pallas as pl
from jax.experimental.pallas import tpu as pltpu
from jax.sharding import PartitionSpec as P

VMEM = pl.BlockSpec(memory_space=pltpu.VMEM)
ANY = pl.BlockSpec(memory_space=pl.ANY)
LOW_VMEM = 12 * 2**20


def low_kernel(low_rank, count, first, row, *refs):
    pieces = refs[:count]
    mine_ref, other_ref, key_ref, acc_ref = refs[count : count + 4]
    out_ref, up_ref, far_ref, sem = refs[-4:]
    half = pieces[0].shape[0] // 2
    d_local = mine_ref.shape[1]
    copies = []
    for n, p in enumerate(pieces):
        for k, table in enumerate((up_ref, far_ref)):
            copies.append(
                pltpu.make_async_copy(
                    p.at[k * half : (k + 1) * half, d_local:],
                    table.at[row + n * half : row + (n + 1) * half],
                    sem.at[2 * n + k],
                )
            )
            copies[-1].start()
    found = lax.dot_general(
        jnp.concatenate([p[:half, :d_local] for p in pieces], axis=0),
        mine_ref[...],
        (((1,), (1,)), ((), ())),
        preferred_element_type=jnp.float32,
    ) + lax.dot_general(
        jnp.concatenate([p[half:, :d_local] for p in pieces], axis=0),
        other_ref[...],
        (((1,), (1,)), ((), ())),
        preferred_element_type=jnp.float32,
    )
    key = key_ref[...]
    total = acc_ref[...]
    for g in range(found.shape[0] // low_rank):
        total = total + jnp.where(
            key == first + g, found[g * low_rank : (g + 1) * low_rank], 0.0
        )
    out_ref[...] = jnp.broadcast_to(total.astype(out_ref.dtype), out_ref.shape)
    for copy in copies:
        copy.wait()


def low_add(low_rank, first, row, pieces, mine, other, key, acc, out, tables, table_shape):
    tok_rows, d_local = mine.shape
    count = len(pieces)
    half = count * pieces[0].shape[0] // 2
    return pl.pallas_call(
        functools.partial(low_kernel, low_rank, count, first, row),
        out_shape=(out, table_shape, table_shape),
        in_specs=[VMEM] * (count + 4) + [ANY] * len(tables),
        out_specs=(VMEM, ANY, ANY),
        scratch_shapes=[pltpu.SemaphoreType.DMA((2 * count,))],
        input_output_aliases={count + 4 + i: 1 + i for i in range(len(tables))},
        cost_estimate=pl.CostEstimate(
            flops=4 * half * d_local * tok_rows,
            bytes_accessed=4 * half * d_local,
            transcendentals=0,
        ),
        compiler_params=pltpu.CompilerParams(vmem_limit_bytes=LOW_VMEM),
    )(*pieces, mine, other, key, acc, *tables)


def base_kernel(width, tokens_ref, weight_ref, out_ref):
    step = 2 * width
    for at in range(0, weight_ref.shape[1], step):
        found = jnp.dot(
            tokens_ref[...], weight_ref[:, at : at + step], preferred_element_type=jnp.float32
        )
        out_ref[at // width] = found[:, :width]
        out_ref[at // width + 1] = found[:, width:]


def base_blocks_of(tokens, weight, width):
    rows, depth = tokens.shape
    return pl.pallas_call(
        functools.partial(base_kernel, width),
        out_shape=jax.ShapeDtypeStruct((weight.shape[1] // width, rows, width), jnp.float32),
        in_specs=[VMEM, VMEM],
        out_specs=VMEM,
        cost_estimate=pl.CostEstimate(
            flops=2 * rows * depth * weight.shape[1],
            bytes_accessed=8 * weight.size,
            transcendentals=0,
        ),
        compiler_params=pltpu.CompilerParams(vmem_limit_bytes=LOW_VMEM),
    )(tokens, weight)


def sum_kernel(blocks_ref, out_ref):
    out_ref[...] = jnp.sum(blocks_ref[...], axis=0)


def sum_blocks(blocks):
    return pl.pallas_call(
        sum_kernel,
        out_shape=jax.ShapeDtypeStruct(blocks.shape[1:], blocks.dtype),
        in_specs=[VMEM],
        out_specs=VMEM,
        cost_estimate=pl.CostEstimate(
            flops=blocks.size, bytes_accessed=4 * blocks.size, transcendentals=0
        ),
        compiler_params=pltpu.CompilerParams(vmem_limit_bytes=LOW_VMEM),
    )(blocks)


def delta_kernel(low_rank, adp_dev, low_ref, key_ref, far_key_ref, up_ref, far_ref, base_ref, out_ref):
    low = jnp.sum(low_ref[...].astype(jnp.float32), axis=0).astype(jnp.bfloat16)
    half = adp_dev // 2 * low_rank
    tile = 4 * half
    acc = jnp.zeros((base_ref.shape[1], base_ref.shape[0]), jnp.float32)
    for key, table in ((key_ref[...], up_ref), (far_key_ref[...], far_ref)):
        for row in range(0, table.shape[0], tile):
            groups = []
            for at in range(row, row + tile, low_rank):
                adapter = at // low_rank + (adp_dev // 2 if at >= half else 0)
                groups.append(low * jnp.where(key == adapter, 1.0, 0.0).astype(jnp.bfloat16))
            acc += lax.dot_general(
                table[row : row + tile],
                jnp.concatenate(groups, axis=0),
                (((0,), (0,)), ((), ())),
                preferred_element_type=jnp.float32,
            )
    delta = acc.astype(jnp.bfloat16).astype(jnp.float32)
    out_ref[...] = (base_ref[...] + delta.T).astype(jnp.bfloat16)


def delta_add(low_rank, adp_dev, low_all, key, far_key, up, far, base):
    tok_rows, kv_local = base.shape
    return pl.pallas_call(
        functools.partial(delta_kernel, low_rank, adp_dev),
        out_shape=jax.ShapeDtypeStruct((tok_rows, kv_local), jnp.bfloat16),
        in_specs=[VMEM] * 6,
        out_specs=VMEM,
        cost_estimate=pl.CostEstimate(
            flops=4 * far.shape[0] * kv_local * tok_rows,
            bytes_accessed=8 * far.shape[0] * kv_local,
            transcendentals=0,
        ),
        compiler_params=pltpu.CompilerParams(vmem_limit_bytes=24 * 2**20),
    )(low_all, key, far_key, up, far, base)


def per_device(tokens, adapter_ids, value_weight, adapter_down, adapter_up):
    tok_rows, d_local = tokens.shape
    n_tok = lax.axis_size("tok")
    n_hid = lax.axis_size("hid")
    adp_dev, low_rank, _ = adapter_down.shape
    kv_local = adapter_up.shape[2]
    rows = adp_dev * low_rank
    half = rows // 2
    half_adp = adp_dev // 2
    f32 = jnp.float32
    me = lax.axis_index("tok")
    side = lax.axis_index("hid") % 2
    token_ids = adapter_ids[:, 0][None, :]

    swap = [(h, h ^ 1) for h in range(n_hid)]
    onward = []
    for t in range(n_tok):
        for h in range(n_hid):
            onward.append((t * n_hid + h, ((t + 1 - 2 * (h % 2)) % n_tok) * n_hid + h))

    block = jnp.concatenate(
        [adapter_down.reshape(rows, d_local), adapter_up.reshape(rows, kv_local)], axis=1
    )
    block_other = lax.ppermute(block, "hid", swap)
    top = jnp.concatenate([block[:half], block_other[:half]], axis=0)
    bottom = jnp.concatenate([block[half:], block_other[half:]], axis=0)
    flight = [jnp.where(side == 0, top, bottom), jnp.where(side == 0, bottom, top)]
    flight[0], flight[1], tokens = lax.optimization_barrier((flight[0], flight[1], tokens))
    own = flight[0]
    tokens_other = lax.ppermute(tokens, "hid", swap)
    owner, slot = token_ids // adp_dev, token_ids % adp_dev
    behind = jnp.where(me >= owner, me - owner, me - owner + n_tok)
    ahead = jnp.where(owner >= me, owner - me, owner - me + n_tok)
    turned = (slot + half_adp) % adp_dev
    key = jnp.where(side == 0, behind * adp_dev + slot, ahead * adp_dev + turned)
    far_key = jnp.where(side == 0, ahead * adp_dev + turned, behind * adp_dev + slot)

    sums = jax.ShapeDtypeStruct((low_rank, tok_rows), f32)
    table_shape = jax.ShapeDtypeStruct((n_tok // 2 * rows, kv_local), jnp.bfloat16)

    def add(state, step, pieces, out=sums):
        low, *tables = state
        row = step * rows - half if step else 0
        return low_add(
            low_rank,
            step * adp_dev,
            row,
            pieces,
            tokens,
            tokens_other,
            key,
            low,
            out,
            tables,
            table_shape,
        )

    def tie(value, *chunks):
        for c in chunks:
            flight[c], value = lax.optimization_barrier((flight[c], value))
        return value

    waiting = []
    state = add((jnp.zeros(sums.shape, f32),), 0, [own])
    for step in range(1, n_tok // 2):
        for c in range(2):
            flight[c] = lax.ppermute(flight[c], ("tok", "hid"), onward)
        waiting += flight
        if step == 1:
            flight[1], value_weight = lax.optimization_barrier((flight[1], value_weight))
            partial_base = base_blocks_of(tokens, value_weight, kv_local)
        if step == 2:
            partial_base = tie(partial_base, 0, 1)
        if step == 4:
            partial_base = tie(partial_base, 0, 1)
            base_blocks = lax.all_to_all(partial_base, "hid", 0, 0, tiled=True)
        if step % 2 == 0 or step == n_tok // 2 - 1:
            if step > 2:
                flight[1], state = lax.optimization_barrier((flight[1], state))
            state = add(state, step - len(waiting) // 2 + 1, waiting)
            waiting = []
        if step == 8:
            base_blocks = tie(base_blocks, 1)
            base = sum_blocks(base_blocks)
        if step == 9:
            base = tie(base, 1)
    last = lax.ppermute(flight[0], ("tok", "hid"), onward)
    low_copies, up, far = add(
        state,
        n_tok // 2,
        [last],
        jax.ShapeDtypeStruct((n_hid, low_rank, tok_rows), jnp.bfloat16),
    )
    low_all = lax.all_to_all(low_copies, "hid", 0, 0, tiled=True)
    far = lax.ppermute(far, "hid", swap)
    return delta_add(low_rank, adp_dev, low_all, key, far_key, up, far, base)


def solution(mesh):
    in_specs = (
        P(("parts", "tok"), "hid"),
        P(("parts", "tok"), None),
        P("hid", None),
        P("tok", None, "hid"),
        P("tok", None, "hid"),
    )
    out_specs = P(("parts", "tok"), "hid")
    return jax.shard_map(
        per_device, mesh=mesh, in_specs=in_specs, out_specs=out_specs, check_vma=False
    )
```

```python
import functools

import jax
import jax.numpy as jnp
from jax import lax
from jax.experimental import pallas as pl
from jax.experimental.pallas import tpu as pltpu
from jax.sharding import PartitionSpec as P


VMEM = pl.BlockSpec(memory_space=pltpu.VMEM)
ANY = pl.BlockSpec(memory_space=pl.ANY)
CHUNKS = 3
LOW_VMEM = 12 * 2**20


def low_kernel(low_rank, steps, used, first, row, *refs):
    pieces = refs[: steps * CHUNKS]
    mine_ref, other_ref, key_ref, acc_ref = refs[steps * CHUNKS : steps * CHUNKS + 4]
    out_ref, up_ref, far_ref, sem = refs[-4:]
    rows, width = pieces[0].shape[0] // 2, pieces[0].shape[1]
    d_local = mine_ref.shape[1]
    copies = []
    for n in range(steps):
        for k, table in enumerate((up_ref, far_ref)):
            copies.append(
                pltpu.make_async_copy(
                    pieces[(n + 1) * CHUNKS - 1].at[
                        k * rows : k * rows + used, width - table.shape[1] :
                    ],
                    table.at[row + n * used : row + (n + 1) * used],
                    sem.at[2 * n + k],
                )
            )
            copies[-1].start()
    found = jnp.zeros((steps * used, mine_ref.shape[0]), jnp.float32)
    for j in range(CHUNKS):
        at, end = j * width, min((j + 1) * width, d_local)
        for k, side_ref in enumerate((mine_ref, other_ref)):
            found += lax.dot_general(
                jnp.concatenate(
                    [
                        pieces[n * CHUNKS + j][k * rows : k * rows + used, : end - at]
                        for n in range(steps)
                    ],
                    axis=0,
                ),
                side_ref[:, at:end],
                (((1,), (1,)), ((), ())),
                preferred_element_type=jnp.float32,
            )
    key = key_ref[...]
    total = acc_ref[...]
    for g in range(found.shape[0] // low_rank):
        total = total + jnp.where(
            key == first + g, found[g * low_rank : (g + 1) * low_rank], 0.0
        )
    out_ref[...] = jnp.broadcast_to(total.astype(out_ref.dtype), out_ref.shape)
    for copy in copies:
        copy.wait()


def low_add(low_rank, first, row, used, pieces, mine, other, key, acc, out, tables, table_shape):
    tok_rows, d_local = mine.shape
    count = len(pieces)
    steps = count // CHUNKS
    return pl.pallas_call(
        functools.partial(low_kernel, low_rank, steps, used, first, row),
        out_shape=(out, table_shape, table_shape),
        in_specs=[VMEM] * (count + 4) + [ANY] * len(tables),
        out_specs=(VMEM, ANY, ANY),
        scratch_shapes=[pltpu.SemaphoreType.DMA((2 * steps,))],
        input_output_aliases={count + 4 + i: 1 + i for i in range(len(tables))},
        cost_estimate=pl.CostEstimate(
            flops=4 * steps * used * d_local * tok_rows,
            bytes_accessed=4 * steps * used * d_local,
            transcendentals=0,
        ),
        compiler_params=pltpu.CompilerParams(vmem_limit_bytes=LOW_VMEM),
    )(*pieces, mine, other, key, acc, *tables)


def base_kernel(width, tokens_ref, weight_ref, out_ref):
    step = 2 * width
    for at in range(0, weight_ref.shape[1], step):
        found = jnp.dot(
            tokens_ref[...], weight_ref[:, at : at + step], preferred_element_type=jnp.float32
        )
        out_ref[at // width] = found[:, :width]
        out_ref[at // width + 1] = found[:, width:]


def base_blocks_of(tokens, weight, width):
    rows, depth = tokens.shape
    return pl.pallas_call(
        functools.partial(base_kernel, width),
        out_shape=jax.ShapeDtypeStruct((weight.shape[1] // width, rows, width), jnp.float32),
        in_specs=[VMEM, VMEM],
        out_specs=VMEM,
        cost_estimate=pl.CostEstimate(
            flops=2 * rows * depth * weight.shape[1],
            bytes_accessed=8 * weight.size,
            transcendentals=0,
        ),
        compiler_params=pltpu.CompilerParams(vmem_limit_bytes=LOW_VMEM),
    )(tokens, weight)


def sum_kernel(blocks_ref, out_ref):
    out_ref[...] = jnp.sum(blocks_ref[...], axis=0)


def sum_blocks(blocks):
    return pl.pallas_call(
        sum_kernel,
        out_shape=jax.ShapeDtypeStruct(blocks.shape[1:], blocks.dtype),
        in_specs=[VMEM],
        out_specs=VMEM,
        cost_estimate=pl.CostEstimate(
            flops=blocks.size, bytes_accessed=4 * blocks.size, transcendentals=0
        ),
        compiler_params=pltpu.CompilerParams(vmem_limit_bytes=LOW_VMEM),
    )(blocks)


def delta_kernel(low_rank, adp_dev, low_ref, key_ref, far_key_ref, up_ref, far_ref, base_ref, out_ref):
    low = jnp.sum(low_ref[...].astype(jnp.float32), axis=0).astype(jnp.bfloat16)
    half = adp_dev // 2 * low_rank
    tile = 4 * half
    acc = jnp.zeros((base_ref.shape[1], base_ref.shape[0]), jnp.float32)
    for key, table in ((key_ref[...], up_ref), (far_key_ref[...], far_ref)):
        for row in range(0, table.shape[0], tile):
            groups = []
            for at in range(row, row + tile, low_rank):
                adapter = at // low_rank + (adp_dev // 2 if at >= half else 0)
                groups.append(low * jnp.where(key == adapter, 1.0, 0.0).astype(jnp.bfloat16))
            acc += lax.dot_general(
                table[row : row + tile],
                jnp.concatenate(groups, axis=0),
                (((0,), (0,)), ((), ())),
                preferred_element_type=jnp.float32,
            )
    delta = acc.astype(jnp.bfloat16).astype(jnp.float32)
    out_ref[...] = (base_ref[...] + delta.T).astype(jnp.bfloat16)


def delta_add(low_rank, adp_dev, low_all, key, far_key, up, far, base):
    tok_rows, kv_local = base.shape
    return pl.pallas_call(
        functools.partial(delta_kernel, low_rank, adp_dev),
        out_shape=jax.ShapeDtypeStruct((tok_rows, kv_local), jnp.bfloat16),
        in_specs=[VMEM] * 6,
        out_specs=VMEM,
        cost_estimate=pl.CostEstimate(
            flops=4 * far.shape[0] * kv_local * tok_rows,
            bytes_accessed=8 * far.shape[0] * kv_local,
            transcendentals=0,
        ),
        compiler_params=pltpu.CompilerParams(vmem_limit_bytes=24 * 2**20),
    )(low_all, key, far_key, up, far, base)


def per_device(tokens, adapter_ids, value_weight, adapter_down, adapter_up):
    tok_rows, d_local = tokens.shape
    n_tok = lax.axis_size("tok")
    n_hid = lax.axis_size("hid")
    adp_dev, low_rank, _ = adapter_down.shape
    kv_local = adapter_up.shape[2]
    rows = adp_dev * low_rank
    half = rows // 2
    half_adp = adp_dev // 2
    f32 = jnp.float32
    me = lax.axis_index("tok")
    side = lax.axis_index("hid") % 2
    token_ids = adapter_ids[:, 0][None, :]

    swap = [(h, h ^ 1) for h in range(n_hid)]
    onward = []
    for t in range(n_tok):
        for h in range(n_hid):
            onward.append((t * n_hid + h, ((t + 1 - 2 * (h % 2)) % n_tok) * n_hid + h))

    block = jnp.concatenate(
        [adapter_down.reshape(rows, d_local), adapter_up.reshape(rows, kv_local)], axis=1
    )
    block_other = lax.ppermute(block, "hid", swap)

    def ordered(array):
        return jnp.where(side == 0, array, jnp.concatenate([array[half:], array[:half]], axis=0))

    both = jnp.concatenate([ordered(block), ordered(block_other)], axis=0)
    width = both.shape[1] // CHUNKS
    flight = [both[:, c * width : (c + 1) * width] for c in range(CHUNKS)]
    *flight, tokens = lax.optimization_barrier((*flight, tokens))
    own = list(flight)
    tokens_other = lax.ppermute(tokens, "hid", swap)
    owner, slot = token_ids // adp_dev, token_ids % adp_dev
    behind = jnp.where(me >= owner, me - owner, me - owner + n_tok)
    ahead = jnp.where(owner >= me, owner - me, owner - me + n_tok)
    turned = (slot + half_adp) % adp_dev
    key = jnp.where(side == 0, behind * adp_dev + slot, ahead * adp_dev + turned)
    far_key = jnp.where(side == 0, ahead * adp_dev + turned, behind * adp_dev + slot)

    sums = jax.ShapeDtypeStruct((low_rank, tok_rows), f32)
    table_shape = jax.ShapeDtypeStruct((n_tok // 2 * rows, kv_local), jnp.bfloat16)

    def add(state, step, pieces, used=rows, out=sums):
        low, *tables = state
        row = step * rows - half if step else 0
        return low_add(
            low_rank,
            step * adp_dev,
            row,
            used,
            pieces,
            tokens,
            tokens_other,
            key,
            low,
            out,
            tables,
            table_shape,
        )

    def hop():
        for c in range(CHUNKS):
            flight[c] = lax.ppermute(flight[c], ("tok", "hid"), onward)

    def tie(value, *chunks):
        for c in chunks:
            flight[c], value = lax.optimization_barrier((flight[c], value))
        return value

    waiting = []
    last = CHUNKS - 1
    state = add((jnp.zeros(sums.shape, f32),), 0, own, half)
    for step in range(1, n_tok // 2):
        hop()
        waiting += flight
        if step == 2:
            value_weight = tie(value_weight, last)
            partial_base = base_blocks_of(tokens, value_weight, kv_local)
        if step == 3:
            partial_base = tie(partial_base, last)
        if step == 4:
            base_blocks = lax.all_to_all(partial_base, "hid", 0, 0, tiled=True)
        if step % 2 == 0 or step == n_tok // 2 - 1:
            if step > 2:
                flight[last], state = lax.optimization_barrier((flight[last], state))
            state = add(state, step - len(waiting) // CHUNKS + 1, waiting)
            waiting = []
        if step == 10:
            base_blocks = tie(base_blocks, last)
            base = sum_blocks(base_blocks)
        if step == 11:
            base = tie(base, last)
    hop()
    low_copies, up, far = add(
        state,
        n_tok // 2,
        flight,
        half,
        jax.ShapeDtypeStruct((n_hid, low_rank, tok_rows), jnp.bfloat16),
    )
    low_all = lax.all_to_all(low_copies, "hid", 0, 0, tiled=True)
    far = lax.ppermute(far, "hid", swap)
    return delta_add(low_rank, adp_dev, low_all, key, far_key, up, far, base)


def solution(mesh):
    in_specs = (
        P(("parts", "tok"), "hid"),
        P(("parts", "tok"), None),
        P("hid", None),
        P("tok", None, "hid"),
        P("tok", None, "hid"),
    )
    out_specs = P(("parts", "tok"), "hid")

    return jax.shard_map(
        per_device, mesh=mesh, in_specs=in_specs, out_specs=out_specs, check_vma=False
    )
```

```python
import functools

import jax
import jax.numpy as jnp
from jax import lax
from jax.experimental import pallas as pl
from jax.experimental.pallas import tpu as pltpu
from jax.sharding import PartitionSpec as P


VMEM = pl.BlockSpec(memory_space=pltpu.VMEM)
LOW_VMEM = 12 * 2**20


def low_kernel(low_rank, count, first, *refs):
    pieces = refs[:count]
    mine_ref, other_ref, key_ref, acc_ref, out_ref = refs[count:]
    half = pieces[0].shape[0] // 2
    found = lax.dot_general(
        jnp.concatenate([p[:half, :] for p in pieces], axis=0),
        mine_ref[...],
        (((1,), (1,)), ((), ())),
        preferred_element_type=jnp.float32,
    ) + lax.dot_general(
        jnp.concatenate([p[half:, :] for p in pieces], axis=0),
        other_ref[...],
        (((1,), (1,)), ((), ())),
        preferred_element_type=jnp.float32,
    )
    key = key_ref[...]
    total = acc_ref[...]
    for g in range(found.shape[0] // low_rank):
        total = total + jnp.where(
            key == first + g, found[g * low_rank : (g + 1) * low_rank], 0.0
        )
    out_ref[...] = jnp.broadcast_to(total.astype(out_ref.dtype), out_ref.shape)


def low_add(low_rank, first, pieces, mine, other, key, acc, out):
    tok_rows, d_local = mine.shape
    count = len(pieces)
    half = count * pieces[0].shape[0] // 2
    return pl.pallas_call(
        functools.partial(low_kernel, low_rank, count, first),
        out_shape=out,
        in_specs=[VMEM] * (count + 4),
        out_specs=VMEM,
        cost_estimate=pl.CostEstimate(
            flops=4 * half * d_local * tok_rows,
            bytes_accessed=4 * half * d_local,
            transcendentals=0,
        ),
        compiler_params=pltpu.CompilerParams(vmem_limit_bytes=LOW_VMEM),
    )(*pieces, mine, other, key, acc)


def base_kernel(width, tokens_ref, weight_ref, out_ref):
    step = 2 * width
    for at in range(0, weight_ref.shape[1], step):
        found = jnp.dot(
            tokens_ref[...], weight_ref[:, at : at + step], preferred_element_type=jnp.float32
        )
        out_ref[at // width] = found[:, :width]
        out_ref[at // width + 1] = found[:, width:]


def base_blocks_of(tokens, weight, width):
    rows, depth = tokens.shape
    return pl.pallas_call(
        functools.partial(base_kernel, width),
        out_shape=jax.ShapeDtypeStruct((weight.shape[1] // width, rows, width), jnp.float32),
        in_specs=[VMEM, VMEM],
        out_specs=VMEM,
        cost_estimate=pl.CostEstimate(
            flops=2 * rows * depth * weight.shape[1],
            bytes_accessed=8 * weight.size,
            transcendentals=0,
        ),
        compiler_params=pltpu.CompilerParams(vmem_limit_bytes=LOW_VMEM),
    )(tokens, weight)


def sum_kernel(blocks_ref, out_ref):
    out_ref[...] = jnp.sum(blocks_ref[...], axis=0)


def sum_blocks(blocks):
    return pl.pallas_call(
        sum_kernel,
        out_shape=jax.ShapeDtypeStruct(blocks.shape[1:], blocks.dtype),
        in_specs=[VMEM],
        out_specs=VMEM,
        cost_estimate=pl.CostEstimate(
            flops=blocks.size, bytes_accessed=4 * blocks.size, transcendentals=0
        ),
        compiler_params=pltpu.CompilerParams(vmem_limit_bytes=LOW_VMEM),
    )(blocks)


def delta_kernel(low_rank, low_ref, ids_ref, up_ref, base_ref, out_ref):
    low = jnp.sum(low_ref[...].astype(jnp.float32), axis=0).astype(jnp.bfloat16)
    ids = ids_ref[...]
    tile = 16 * low_rank
    acc = jnp.zeros((base_ref.shape[1], base_ref.shape[0]), jnp.float32)
    for row in range(0, up_ref.shape[0], tile):
        groups = [
            low * jnp.where(ids == at // low_rank, 1.0, 0.0).astype(jnp.bfloat16)
            for at in range(row, row + tile, low_rank)
        ]
        acc += lax.dot_general(
            up_ref[row : row + tile],
            jnp.concatenate(groups, axis=0),
            (((0,), (0,)), ((), ())),
            preferred_element_type=jnp.float32,
        )
    delta = acc.astype(jnp.bfloat16).astype(jnp.float32)
    out_ref[...] = (base_ref[...] + delta.T).astype(jnp.bfloat16)


def delta_add(low_rank, low_all, ids, up, base):
    tok_rows, kv_local = base.shape
    return pl.pallas_call(
        functools.partial(delta_kernel, low_rank),
        out_shape=jax.ShapeDtypeStruct((tok_rows, kv_local), jnp.bfloat16),
        in_specs=[VMEM] * 4,
        out_specs=VMEM,
        cost_estimate=pl.CostEstimate(
            flops=2 * up.shape[0] * kv_local * tok_rows,
            bytes_accessed=4 * up.shape[0] * kv_local,
            transcendentals=0,
        ),
        compiler_params=pltpu.CompilerParams(vmem_limit_bytes=24 * 2**20),
    )(low_all, ids, up, base)


def per_device(tokens, adapter_ids, value_weight, adapter_down, adapter_up):
    tok_rows, d_local = tokens.shape
    n_tok = lax.axis_size("tok")
    n_hid = lax.axis_size("hid")
    adp_dev, low_rank, _ = adapter_down.shape
    kv_local = adapter_up.shape[2]
    rows = adp_dev * low_rank
    half = rows // 2
    half_adp = adp_dev // 2
    f32 = jnp.float32
    me = lax.axis_index("tok")
    side = lax.axis_index("hid") % 2
    token_ids = adapter_ids[:, 0][None, :]

    swap = [(h, h ^ 1) for h in range(n_hid)]
    onward = []
    for t in range(n_tok):
        for h in range(n_hid):
            onward.append((t * n_hid + h, ((t + 1 - 2 * (h % 2)) % n_tok) * n_hid + h))

    up_all = lax.all_gather(adapter_up.reshape(rows, kv_local), "tok", axis=0, tiled=True)
    block = adapter_down.reshape(rows, d_local)
    block_other = lax.ppermute(block, "hid", swap)
    top = jnp.concatenate([block[:half], block_other[:half]], axis=0)
    bottom = jnp.concatenate([block[half:], block_other[half:]], axis=0)
    flight = [jnp.where(side == 0, top, bottom), jnp.where(side == 0, bottom, top)]
    flight[0], flight[1], tokens = lax.optimization_barrier((flight[0], flight[1], tokens))
    own = flight[0]
    tokens_other = lax.ppermute(tokens, "hid", swap)
    owner, slot = token_ids // adp_dev, token_ids % adp_dev
    behind = jnp.where(me >= owner, me - owner, me - owner + n_tok)
    ahead = jnp.where(owner >= me, owner - me, owner - me + n_tok)
    turned = (slot + half_adp) % adp_dev
    key = jnp.where(side == 0, behind * adp_dev + slot, ahead * adp_dev + turned)

    sums = jax.ShapeDtypeStruct((low_rank, tok_rows), f32)

    def add(low, step, pieces, out=sums):
        return low_add(
            low_rank, step * adp_dev, pieces, tokens, tokens_other, key, low, out
        )

    def tie(value, *chunks):
        for c in chunks:
            flight[c], value = lax.optimization_barrier((flight[c], value))
        return value

    waiting = []
    state = add(jnp.zeros(sums.shape, f32), 0, [own])
    for step in range(1, n_tok // 2):
        for c in range(2):
            flight[c] = lax.ppermute(flight[c], ("tok", "hid"), onward)
        waiting += flight
        if step == 2:
            value_weight = tie(value_weight, 1)
            partial_base = base_blocks_of(tokens, value_weight, kv_local)
        if step == 3:
            partial_base = tie(partial_base, 1)
        if step == 4:
            base_blocks = lax.all_to_all(partial_base, "hid", 0, 0, tiled=True)
        if step % 2 == 0 or step == n_tok // 2 - 1:
            if step > 2:
                flight[1], state = lax.optimization_barrier((flight[1], state))
            state = add(state, step - len(waiting) // 2 + 1, waiting)
            waiting = []
        if step == 10:
            base_blocks = tie(base_blocks, 1)
            base = sum_blocks(base_blocks)
        if step == 11:
            base = tie(base, 1)
    last = lax.ppermute(flight[0], ("tok", "hid"), onward)
    low_copies = add(
        state,
        n_tok // 2,
        [last],
        jax.ShapeDtypeStruct((n_hid, low_rank, tok_rows), jnp.bfloat16),
    )
    low_all = lax.all_to_all(low_copies, "hid", 0, 0, tiled=True)
    return delta_add(low_rank, low_all, token_ids, up_all, base)


def solution(mesh):
    in_specs = (
        P(("parts", "tok"), "hid"),
        P(("parts", "tok"), None),
        P("hid", None),
        P("tok", None, "hid"),
        P("tok", None, "hid"),
    )
    out_specs = P(("parts", "tok"), "hid")

    return jax.shard_map(
        per_device, mesh=mesh, in_specs=in_specs, out_specs=out_specs, check_vma=False
    )
```

```python
import functools

import jax
import jax.numpy as jnp
from jax import lax
from jax.experimental import pallas as pl
from jax.experimental.pallas import tpu as pltpu
from jax.sharding import PartitionSpec as P


VMEM = pl.BlockSpec(memory_space=pltpu.VMEM)
ANY = pl.BlockSpec(memory_space=pl.ANY)
LOW_VMEM = 12 * 2**20


def low_kernel(low_rank, count, first, row, *refs):
    pieces = refs[:count]
    mine_ref, other_ref, key_ref, acc_ref = refs[count : count + 4]
    out_ref, up_ref, far_ref, sem = refs[-4:]
    half = pieces[0].shape[0] // 2
    d_local = mine_ref.shape[1]
    copies = []
    for n, p in enumerate(pieces):
        for k, table in enumerate((up_ref, far_ref)):
            copies.append(
                pltpu.make_async_copy(
                    p.at[k * half : (k + 1) * half, d_local:],
                    table.at[row + n * half : row + (n + 1) * half],
                    sem.at[2 * n + k],
                )
            )
            copies[-1].start()
    found = lax.dot_general(
        jnp.concatenate([p[:half, :d_local] for p in pieces], axis=0),
        mine_ref[...],
        (((1,), (1,)), ((), ())),
        preferred_element_type=jnp.float32,
    ) + lax.dot_general(
        jnp.concatenate([p[half:, :d_local] for p in pieces], axis=0),
        other_ref[...],
        (((1,), (1,)), ((), ())),
        preferred_element_type=jnp.float32,
    )
    key = key_ref[...]
    total = acc_ref[...]
    for g in range(found.shape[0] // low_rank):
        total = total + jnp.where(
            key == first + g, found[g * low_rank : (g + 1) * low_rank], 0.0
        )
    out_ref[...] = jnp.broadcast_to(total.astype(out_ref.dtype), out_ref.shape)
    for copy in copies:
        copy.wait()


def low_add(low_rank, first, row, pieces, mine, other, key, acc, out, tables, table_shape):
    tok_rows, d_local = mine.shape
    count = len(pieces)
    half = count * pieces[0].shape[0] // 2
    return pl.pallas_call(
        functools.partial(low_kernel, low_rank, count, first, row),
        out_shape=(out, table_shape, table_shape),
        in_specs=[VMEM] * (count + 4) + [ANY] * len(tables),
        out_specs=(VMEM, ANY, ANY),
        scratch_shapes=[pltpu.SemaphoreType.DMA((2 * count,))],
        input_output_aliases={count + 4 + i: 1 + i for i in range(len(tables))},
        cost_estimate=pl.CostEstimate(
            flops=4 * half * d_local * tok_rows,
            bytes_accessed=4 * half * d_local,
            transcendentals=0,
        ),
        compiler_params=pltpu.CompilerParams(vmem_limit_bytes=LOW_VMEM),
    )(*pieces, mine, other, key, acc, *tables)


def base_kernel(width, tokens_ref, weight_ref, out_ref):
    step = 2 * width
    for at in range(0, weight_ref.shape[1], step):
        found = jnp.dot(
            tokens_ref[...], weight_ref[:, at : at + step], preferred_element_type=jnp.float32
        )
        out_ref[at // width] = found[:, :width]
        out_ref[at // width + 1] = found[:, width:]


def base_blocks_of(tokens, weight, width):
    rows, depth = tokens.shape
    return pl.pallas_call(
        functools.partial(base_kernel, width),
        out_shape=jax.ShapeDtypeStruct((weight.shape[1] // width, rows, width), jnp.float32),
        in_specs=[VMEM, VMEM],
        out_specs=VMEM,
        cost_estimate=pl.CostEstimate(
            flops=2 * rows * depth * weight.shape[1],
            bytes_accessed=8 * weight.size,
            transcendentals=0,
        ),
        compiler_params=pltpu.CompilerParams(vmem_limit_bytes=LOW_VMEM),
    )(tokens, weight)


def sum_kernel(blocks_ref, out_ref):
    out_ref[...] = jnp.sum(blocks_ref[...], axis=0)


def sum_blocks(blocks):
    return pl.pallas_call(
        sum_kernel,
        out_shape=jax.ShapeDtypeStruct(blocks.shape[1:], blocks.dtype),
        in_specs=[VMEM],
        out_specs=VMEM,
        cost_estimate=pl.CostEstimate(
            flops=blocks.size, bytes_accessed=4 * blocks.size, transcendentals=0
        ),
        compiler_params=pltpu.CompilerParams(vmem_limit_bytes=LOW_VMEM),
    )(blocks)


def delta_kernel(low_rank, adp_dev, low_ref, key_ref, far_key_ref, up_ref, far_ref, base_ref, out_ref):
    low = jnp.sum(low_ref[...].astype(jnp.float32), axis=0).astype(jnp.bfloat16)
    half = adp_dev // 2 * low_rank
    tile = 4 * half
    acc = jnp.zeros((base_ref.shape[1], base_ref.shape[0]), jnp.float32)
    for key, table in ((key_ref[...], up_ref), (far_key_ref[...], far_ref)):
        for row in range(0, table.shape[0], tile):
            groups = []
            for at in range(row, row + tile, low_rank):
                adapter = at // low_rank + (adp_dev // 2 if at >= half else 0)
                groups.append(low * jnp.where(key == adapter, 1.0, 0.0).astype(jnp.bfloat16))
            acc += lax.dot_general(
                table[row : row + tile],
                jnp.concatenate(groups, axis=0),
                (((0,), (0,)), ((), ())),
                preferred_element_type=jnp.float32,
            )
    delta = acc.astype(jnp.bfloat16).astype(jnp.float32)
    out_ref[...] = (base_ref[...] + delta.T).astype(jnp.bfloat16)


def delta_add(low_rank, adp_dev, low_all, key, far_key, up, far, base):
    tok_rows, kv_local = base.shape
    return pl.pallas_call(
        functools.partial(delta_kernel, low_rank, adp_dev),
        out_shape=jax.ShapeDtypeStruct((tok_rows, kv_local), jnp.bfloat16),
        in_specs=[VMEM] * 6,
        out_specs=VMEM,
        cost_estimate=pl.CostEstimate(
            flops=4 * far.shape[0] * kv_local * tok_rows,
            bytes_accessed=8 * far.shape[0] * kv_local,
            transcendentals=0,
        ),
        compiler_params=pltpu.CompilerParams(vmem_limit_bytes=24 * 2**20),
    )(low_all, key, far_key, up, far, base)


def per_device(tokens, adapter_ids, value_weight, adapter_down, adapter_up):
    tok_rows, d_local = tokens.shape
    n_tok = lax.axis_size("tok")
    n_hid = lax.axis_size("hid")
    adp_dev, low_rank, _ = adapter_down.shape
    kv_local = adapter_up.shape[2]
    rows = adp_dev * low_rank
    half = rows // 2
    half_adp = adp_dev // 2
    f32 = jnp.float32
    me = lax.axis_index("tok")
    side = lax.axis_index("hid") % 2
    token_ids = adapter_ids[:, 0][None, :]

    swap = [(h, h ^ 1) for h in range(n_hid)]
    onward = []
    for t in range(n_tok):
        for h in range(n_hid):
            onward.append((t * n_hid + h, ((t + 1 - 2 * (h % 2)) % n_tok) * n_hid + h))

    block = jnp.concatenate(
        [adapter_down.reshape(rows, d_local), adapter_up.reshape(rows, kv_local)], axis=1
    )
    block_other = lax.ppermute(block, "hid", swap)
    top = jnp.concatenate([block[:half], block_other[:half]], axis=0)
    bottom = jnp.concatenate([block[half:], block_other[half:]], axis=0)
    flight = [jnp.where(side == 0, top, bottom), jnp.where(side == 0, bottom, top)]
    flight[0], flight[1], tokens = lax.optimization_barrier((flight[0], flight[1], tokens))
    own = flight[0]
    tokens_other = lax.ppermute(tokens, "hid", swap)
    owner, slot = token_ids // adp_dev, token_ids % adp_dev
    behind = jnp.where(me >= owner, me - owner, me - owner + n_tok)
    ahead = jnp.where(owner >= me, owner - me, owner - me + n_tok)
    turned = (slot + half_adp) % adp_dev
    key = jnp.where(side == 0, behind * adp_dev + slot, ahead * adp_dev + turned)
    far_key = jnp.where(side == 0, ahead * adp_dev + turned, behind * adp_dev + slot)

    sums = jax.ShapeDtypeStruct((low_rank, tok_rows), f32)
    table_shape = jax.ShapeDtypeStruct((n_tok // 2 * rows, kv_local), jnp.bfloat16)

    def add(state, step, pieces, out=sums):
        low, *tables = state
        row = step * rows - half if step else 0
        return low_add(
            low_rank,
            step * adp_dev,
            row,
            pieces,
            tokens,
            tokens_other,
            key,
            low,
            out,
            tables,
            table_shape,
        )

    def tie(value, *chunks):
        for c in chunks:
            flight[c], value = lax.optimization_barrier((flight[c], value))
        return value

    waiting = []
    state = add((jnp.zeros(sums.shape, f32),), 0, [own])
    for step in range(1, n_tok // 2):
        for c in range(2):
            flight[c] = lax.ppermute(flight[c], ("tok", "hid"), onward)
        waiting += flight
        if step == 2:
            value_weight = tie(value_weight, 1)
            partial_base = base_blocks_of(tokens, value_weight, kv_local)
        if step == 3:
            partial_base = tie(partial_base, 1)
        if step == 4:
            base_blocks = lax.all_to_all(partial_base, "hid", 0, 0, tiled=True)
        if step % 2 == 0 or step == n_tok // 2 - 1:
            if step > 2:
                flight[1], state = lax.optimization_barrier((flight[1], state))
            state = add(state, step - len(waiting) // 2 + 1, waiting)
            waiting = []
        if step == 10:
            base_blocks = tie(base_blocks, 1)
            base = sum_blocks(base_blocks)
        if step == 11:
            base = tie(base, 1)
    last = lax.ppermute(flight[0], ("tok", "hid"), onward)
    low_copies, up, far = add(
        state,
        n_tok // 2,
        [last],
        jax.ShapeDtypeStruct((n_hid, low_rank, tok_rows), f32),
    )
    low_all = lax.all_to_all(low_copies, "hid", 0, 0, tiled=True)
    far = lax.ppermute(far, "hid", swap)
    return delta_add(low_rank, adp_dev, low_all, key, far_key, up, far, base)


def solution(mesh):
    in_specs = (
        P(("parts", "tok"), "hid"),
        P(("parts", "tok"), None),
        P("hid", None),
        P("tok", None, "hid"),
        P("tok", None, "hid"),
    )
    out_specs = P(("parts", "tok"), "hid")

    return jax.shard_map(
        per_device, mesh=mesh, in_specs=in_specs, out_specs=out_specs, check_vma=False
    )
```
